32 devices in a mesh: sector: 8 (over y, x, core), row: 4 (over z).
Axes of the slice: x: 2, y: 2, z: 4, core: 2. Of those that a mesh axis runs over, the one named last changes fastest.
Arguments:
- psi_sectors: bfloat16 [32, 8192, 256], P('sector', 'row'), may hold values from -1.5 to 1.5
- stiff_blocks: bfloat16 [64, 5, 128, 128], P('row'), as said below
- mass_blocks: bfloat16 [64, 5, 128, 128], P('row'), as said below
- harmonic_table: int32 [16], replicated, may hold values from 0 to 15, each once
Outputs:
- reduced_stiffness: float32 [16, 512, 512], P('sector', 'row')
- reduced_mass: float32 [16, 512, 512], P('sector', 'row')
The draws below stay inside these ranges and needn't reach their ends.
Inputs may be any that keep to these rules, and one draw needn't show every extreme that they name: The stiffness is symmetric: stiff_blocks[i, 2 + d] is the transpose of stiff_blocks[i + d, 2 - d], and blocks whose column lies outside 0 to 63 are zero. `mass_blocks`: the mass is symmetric in the same way, and diagonally dominant with a positive diagonal, hence positive definite.
All inputs are finite; a program needn't handle non-finite values.
Results may differ from the reference program's by a relative error of at most 0.0049.
Values may be sent and summed in bfloat16 or wider, within the bound.
A program may use at most 128 MiB of HBM per device.

```python
import math
import jax
import jax.numpy as jnp
from jax import lax

M = 256
B = 128
REACH = 2
NBAND = 5
SECTORS = 32
SLOTS = 16
DOF = 8192
NBLK = 64


def build_band(key, entry_scale):
    upper_part = jnp.clip(jax.random.normal(key, (NBLK, REACH + 1, B, B), jnp.float32), -6.0, 6.0) * entry_scale
    middle = (upper_part[:, 0] + jnp.swapaxes(upper_part[:, 0], 1, 2)) * 0.5 ** 0.5
    block_ids = jnp.arange(NBLK, dtype=jnp.int32)[:, None, None]
    columns = []
    for offset in range(-REACH, REACH + 1):
        if offset == 0:
            columns.append(middle)
        elif offset > 0:
            inside = block_ids + offset < NBLK
            columns.append(jnp.where(inside, upper_part[:, offset], 0.0))
        else:
            distance = -offset
            flipped = jnp.swapaxes(upper_part[:, distance], 1, 2)
            shifted = jnp.concatenate([jnp.zeros((distance, B, B), jnp.float32), flipped[:NBLK - distance]], axis=0)
            columns.append(shifted)
    return jnp.stack(columns, axis=1)


def draw_stiff_blocks(key, part):
    band = build_band(jax.random.fold_in(key, 11), (NBAND * B) ** (-0.5))
    return band.astype(jnp.bfloat16)


def draw_mass_blocks(key, part):
    band = build_band(jax.random.fold_in(key, 23), 1.0 / (NBAND * B))
    identity = jnp.eye(B, dtype=jnp.float32)
    own_diagonal = jnp.abs(jnp.diagonal(band[:, REACH], axis1=1, axis2=2))
    off_sum = jnp.sum(jnp.abs(band), axis=(1, 3)) - own_diagonal
    factor = jax.random.uniform(jax.random.fold_in(key, 29), (NBLK, B), jnp.float32, 1.1, 2.0)
    new_diagonal = off_sum * factor
    centre = band[:, REACH] * (1.0 - identity) + new_diagonal[:, :, None] * identity
    band = band.at[:, REACH].set(centre)
    return band.astype(jnp.bfloat16)


def block_scale(key, dims, cuts, smallest, largest):
    level = 1.0
    for position, parts in cuts:
        steps = jax.random.uniform(jax.random.fold_in(jax.random.fold_in(key, 6), position), (parts,), jnp.float32, smallest / len(cuts), largest / len(cuts))
        level = level * jnp.repeat(jnp.exp(steps), dims[position] // parts).reshape((-1,) + (1,) * (len(dims) - 1 - position))
    return level


def gaussian(rng, extent, spread, reach, split=(), kind=jnp.bfloat16):
    entries = jax.random.normal(rng, extent, jnp.float32) * spread
    if len(split) > 0:
        entries = block_scale(rng, extent, split, -0.22, 0.18) * entries
    return jnp.clip(entries, min=-reach, max=reach).astype(kind)


def setup_inputs(seed: int = 0) -> dict:
    streams_of = jax.random.split(jax.random.key(seed), 5)
    return {
        "psi_sectors": gaussian(streams_of[0], (SECTORS, DOF, M), (DOF ** -0.25), 1.5, ((0, 8), (1, 4))),
        "stiff_blocks": draw_stiff_blocks(jax.random.fold_in(streams_of[4], 71), 0),
        "mass_blocks": draw_mass_blocks(jax.random.fold_in(streams_of[4], 71), 0),
        "harmonic_table": jax.random.permutation(streams_of[3], SLOTS).astype(jnp.int32),
    }


def coefficients(harmonic_table, sectors_all):
    sector_ids = jnp.arange(sectors_all, dtype=jnp.int32)
    pair_table = harmonic_table.astype(jnp.int32)
    half_count = sectors_all // 2
    second_freq = jnp.where(pair_table == 0, half_count, pair_table)
    first_phase = pair_table[:, None] * sector_ids[None, :] % sectors_all
    second_phase = second_freq[:, None] * sector_ids[None, :] % sectors_all
    angle_unit = 2.0 * math.pi / sectors_all
    first_angle = first_phase.astype(jnp.float32) * angle_unit
    second_angle = second_phase.astype(jnp.float32) * angle_unit
    zero_pair = (pair_table == 0)[:, None]
    low_scale = math.sqrt(1.0 / sectors_all)
    high_scale = math.sqrt(2.0 / sectors_all)
    first_row = jnp.where(zero_pair, low_scale, high_scale) * jnp.cos(first_angle)
    second = jnp.where(zero_pair, low_scale * jnp.cos(second_angle), high_scale * jnp.sin(second_angle))
    return jnp.stack([first_row, second], axis=1).reshape(2 * pair_table.shape[0], sectors_all)

def band_apply(blocks, harmonic):
    block_rows = blocks.shape[0]
    band_count = blocks.shape[1]
    padded = jnp.pad(harmonic.reshape(block_rows, B, harmonic.shape[1]), ((REACH, REACH), (0, 0), (0, 0)))
    block_index = jnp.arange(block_rows, dtype=jnp.int32)[:, None] + jnp.arange(band_count, dtype=jnp.int32)[None, :]
    gathered = padded[block_index].astype(jnp.float32)
    images = jnp.einsum('ijab,ijbm->iam', blocks.astype(jnp.float32), gathered)
    return images.reshape(harmonic.shape).astype(jnp.bfloat16)

def reference(psi_sectors, stiff_blocks, mass_blocks, harmonic_table):
    sectors_all = psi_sectors.shape[0]
    dof_count = psi_sectors.shape[1]
    mode_count = psi_sectors.shape[2]
    dft_table = coefficients(harmonic_table, sectors_all)
    flattened = psi_sectors.reshape(sectors_all, dof_count * mode_count).astype(jnp.float32)
    harmonics = jnp.dot(dft_table, flattened, precision=lax.Precision.HIGHEST).astype(jnp.bfloat16)
    harmonics = harmonics.reshape(sectors_all // 2, 2, dof_count, mode_count)

    def one_slot(pair_field):
        left_basis = jnp.concatenate([pair_field[0], pair_field[1]], axis=1)
        stiff_wide = jnp.concatenate([band_apply(stiff_blocks, pair_field[0]), band_apply(stiff_blocks, pair_field[1])], axis=1)
        mass_wide = jnp.concatenate([band_apply(mass_blocks, pair_field[0]), band_apply(mass_blocks, pair_field[1])], axis=1)
        return (jnp.dot(left_basis.T, stiff_wide, preferred_element_type=jnp.float32), jnp.dot(left_basis.T, mass_wide, preferred_element_type=jnp.float32))
    reduced_stiffness, reduced_mass = lax.map(one_slot, harmonics)
    return (reduced_stiffness, reduced_mass)
```

```python
import functools
import math

import jax
import jax.numpy as jnp
from jax import lax
from jax.experimental import pallas as pl
from jax.experimental.pallas import tpu as pltpu
from jax.sharding import PartitionSpec as P

MESH = pl.DeviceIdType.MESH
LANES = 128
PACK = 16
CHUNKS = 4


def coefficients(harmonic_table, sectors_all):
    sector_ids = jnp.arange(sectors_all, dtype=jnp.int32)
    half_count = sectors_all // 2
    second_freq = jnp.where(harmonic_table == 0, half_count, harmonic_table)
    first_phase = harmonic_table[:, None] * sector_ids[None, :] % sectors_all
    second_phase = second_freq[:, None] * sector_ids[None, :] % sectors_all
    angle_unit = 2.0 * math.pi / sectors_all
    first_angle = first_phase.astype(jnp.float32) * angle_unit
    second_angle = second_phase.astype(jnp.float32) * angle_unit
    zero_pair = (harmonic_table == 0)[:, None]
    low_scale = math.sqrt(1.0 / sectors_all)
    high_scale = math.sqrt(2.0 / sectors_all)
    first_row = jnp.where(zero_pair, low_scale, high_scale) * jnp.cos(first_angle)
    second = jnp.where(
        zero_pair, low_scale * jnp.cos(second_angle), high_scale * jnp.sin(second_angle)
    )
    return jnp.stack([first_row, second], axis=1)


def flipped(index, step, count):
    total, bit = 0, 1
    while bit < count:
        total = total + bit * lax.rem(lax.div(index, bit) + (step // bit) % 2, 2)
        bit *= 2
    return total


def kernel(cfg, table_ref, psi_ref, stiff_ref, mass_ref, out_k, out_m,
           x_buf, h_buf, p_buf, pt_buf, y_buf, band, g_f32, g_send, g_recv, weights,
           s1, r1, l1, s2, r2, l2, sh, rh, s3, r3, lb):
    n, zn, sec, rows, modes, nblk, nband, blk = cfg
    slots = sec // 2
    part = rows // n
    chunk = part // CHUNKS
    halo = (nband // 2) * blk
    total = 2 * modes
    own_rows = total // zn
    d = lax.axis_index("sector")
    z = lax.axis_index("row")
    order = [j for j in (2, 4, 6, 3, 5, 7) if j < n] + [1]
    order += [j for j in range(1, n) if j not in order]

    barrier = pltpu.get_barrier_semaphore()
    for j in order:
        pl.semaphore_signal(barrier, inc=1, device_id={"sector": flipped(d, j, n)}, device_id_type=MESH)
    for j in range(1, zn):
        pl.semaphore_signal(barrier, inc=1, device_id={"row": lax.rem(z + j, zn)}, device_id_type=MESH)
    pl.semaphore_wait(barrier, n - 1 + zn - 1)

    def first(q, j):
        target = flipped(d, j, n)
        return pltpu.make_async_remote_copy(
            src_ref=psi_ref.at[:, pl.ds(target * part + q * chunk, chunk), :],
            dst_ref=x_buf.at[q, pl.ds(d * sec, sec)],
            send_sem=s1.at[q, j], recv_sem=r1.at[q, j],
            device_id={"sector": target}, device_id_type=MESH)

    def first_own(q):
        return pltpu.make_async_copy(
            psi_ref.at[:, pl.ds(d * part + q * chunk, chunk), :],
            x_buf.at[q, pl.ds(d * sec, sec)], l1.at[q])

    def second(q, h, j):
        target = flipped(d, j, n)
        return pltpu.make_async_remote_copy(
            src_ref=h_buf.at[q, h, pl.ds(target * 2, 2)],
            dst_ref=p_buf.at[h, :, pl.ds(halo + d * part + q * chunk, chunk), :],
            send_sem=s2.at[q, h, j], recv_sem=r2.at[q, h, j],
            device_id={"sector": target}, device_id_type=MESH)

    def second_own(q, h):
        return pltpu.make_async_copy(
            h_buf.at[q, h, pl.ds(d * 2, 2)],
            p_buf.at[h, :, pl.ds(halo + d * part + q * chunk, chunk), :], l2.at[q, h])

    def edge(h, up):
        source = rows if up else halo
        dest = 0 if up else halo + rows
        target = lax.rem(z + (1 if up else zn - 1), zn)
        return pltpu.make_async_remote_copy(
            src_ref=p_buf.at[h, :, pl.ds(source, halo), :],
            dst_ref=p_buf.at[h, :, pl.ds(dest, halo), :],
            send_sem=sh.at[h, int(up)], recv_sem=rh.at[h, int(up)],
            device_id={"row": target}, device_id_type=MESH)

    def third(h, j):
        target = lax.rem(z + j, zn)
        return pltpu.make_async_remote_copy(
            src_ref=g_send.at[h, pl.ds(target * own_rows, own_rows), :],
            dst_ref=g_recv.at[h, j - 1],
            send_sem=s3.at[h, j], recv_sem=r3.at[h, j],
            device_id={"row": target}, device_id_type=MESH)

    @pl.loop(0, CHUNKS)
    def _(q):
        for j in order:
            first(q, j).start()
        first_own(q).start()

    band_copies = [pltpu.make_async_copy(stiff_ref, band.at[0], lb.at[0]),
                   pltpu.make_async_copy(mass_ref, band.at[1], lb.at[1])]
    for copy in band_copies:
        copy.start()

    @pl.when(z == 0)
    def _():
        for h in range(slots):
            p_buf[h, :, pl.ds(0, halo), :] = jnp.zeros((2, halo, modes), p_buf.dtype)

    @pl.when(z == zn - 1)
    def _():
        for h in range(slots):
            p_buf[h, :, pl.ds(halo + rows, halo), :] = jnp.zeros((2, halo, modes), p_buf.dtype)

    wide_rows, wide_cols = 2 * n * PACK, n * sec * PACK
    spread_rows = (lax.broadcasted_iota(jnp.int32, (wide_rows, LANES), 0) >> 4
                   == lax.broadcasted_iota(jnp.int32, (wide_rows, LANES), 1)).astype(jnp.float32).astype(jnp.bfloat16)
    spread_cols = (lax.broadcasted_iota(jnp.int32, (LANES, wide_cols), 1) >> 4
                   == lax.broadcasted_iota(jnp.int32, (LANES, wide_cols), 0)).astype(jnp.float32).astype(jnp.bfloat16)
    same = ((lax.broadcasted_iota(jnp.int32, (wide_rows, wide_cols), 0) & (PACK - 1))
            == (lax.broadcasted_iota(jnp.int32, (wide_rows, wide_cols), 1) & (PACK - 1)))
    for h in range(slots):
        value = table_ref[h]
        high = value.astype(jnp.bfloat16)
        low = (value - high.astype(jnp.float32)).astype(jnp.bfloat16)
        for index, piece in enumerate((high, low)):
            tall = jnp.dot(spread_rows, piece, preferred_element_type=jnp.float32).astype(jnp.bfloat16)
            full = jnp.dot(tall, spread_cols, preferred_element_type=jnp.float32)
            weights[h, index] = jnp.where(same, full, 0.0).astype(jnp.bfloat16)

    @pl.loop(0, CHUNKS)
    def _(q):
        for j in order:
            first(q, j).wait_recv()
        first_own(q).wait()

        @pl.loop(0, chunk // PACK)
        def _(g):
            at = pl.ds(pl.multiple_of(g * PACK, PACK), PACK)
            x = x_buf[q, :, at, :].reshape(wide_cols, modes)
            for h in range(slots):
                value = (jnp.dot(weights[h, 0], x, preferred_element_type=jnp.float32)
                         + jnp.dot(weights[h, 1], x, preferred_element_type=jnp.float32))
                h_buf[q, h, :, at, :] = value.astype(jnp.bfloat16).reshape(2 * n, PACK, modes)

        for j in order:
            second(q, 0, j).start()
        second_own(q, 0).start()

    for h in range(1, slots):
        @pl.loop(0, CHUNKS)
        def _(q):
            for j in order:
                second(q, h, j).start()
            second_own(q, h).start()

    for copy in band_copies:
        copy.wait()

    def block_row(h, i):
        at = pl.ds(pl.multiple_of(i * blk, blk), blk)
        blocks = jnp.concatenate(
            [jnp.concatenate([band[which, i, k] for k in range(nband)], axis=1) for which in range(2)], axis=0)
        window = pl.ds(pl.multiple_of(i * blk, blk), nband * blk)
        inner = pl.ds(pl.multiple_of(i * blk + halo, blk), blk)
        for k in range(2):
            image = jnp.dot(blocks, p_buf[h, k, window, :], preferred_element_type=jnp.float32).astype(jnp.bfloat16)
            y_buf[at, k * modes:(k + 1) * modes] = image[:blk]
            y_buf[at, total + k * modes:total + (k + 1) * modes] = image[blk:]
            pt_buf[k * modes:(k + 1) * modes, at] = p_buf[h, k, inner, :].T

    reach = nband // 2

    @pl.loop(0, slots)
    def _(h):
        @pl.loop(0, CHUNKS)
        def _(q):
            for j in order:
                second(q, h, j).wait_recv()
            second_own(q, h).wait()

        @pl.when(z < zn - 1)
        def _():
            edge(h, True).start()

        @pl.when(z > 0)
        def _():
            edge(h, False).start()

        @pl.loop(reach, nblk - reach)
        def _(i):
            block_row(h, i)

        @pl.when(z > 0)
        def _():
            edge(h, True).wait_recv()

        @pl.when(z < zn - 1)
        def _():
            edge(h, False).wait_recv()

        @pl.loop(0, 2 * reach)
        def _(i):
            block_row(h, lax.rem(i + nblk - reach, nblk))

        @pl.loop(0, 2)
        def _(k):
            at = pl.ds(pl.multiple_of(k * modes, modes), modes)
            for c in range(2 * total // modes):
                value = jnp.dot(pt_buf[at, :], y_buf[:, c * modes:(c + 1) * modes],
                                preferred_element_type=jnp.float32)
                g_f32[at, c * modes:(c + 1) * modes] = value
                g_send[h, at, c * modes:(c + 1) * modes] = value.astype(jnp.bfloat16)

        for j in range(1, zn):
            third(h, j).start()
        mine = pl.ds(pl.multiple_of(z * own_rows, own_rows), own_rows)
        out_k[h] = g_f32[mine, :total]
        out_m[h] = g_f32[mine, total:]

    @pl.loop(0, slots)
    def _(h):
        for j in range(1, zn):
            third(h, j).wait_recv()
        for out, start in ((out_k, 0), (out_m, total)):
            value = out[h]
            for j in range(1, zn):
                value = value + g_recv[h, j - 1, :, start:start + total].astype(jnp.float32)
            out[h] = value

    @pl.loop(0, CHUNKS)
    def _(q):
        for j in order:
            first(q, j).wait_send()
            for h in range(slots):
                second(q, h, j).wait_send()

    @pl.loop(0, slots)
    def _(h):
        for j in range(1, zn):
            third(h, j).wait_send()

        @pl.when(z < zn - 1)
        def _():
            edge(h, True).wait_send()

        @pl.when(z > 0)
        def _():
            edge(h, False).wait_send()


def per_device(psi_sectors, stiff_blocks, mass_blocks, harmonic_table):
    sec, rows, modes = psi_sectors.shape
    nblk, nband, blk, _ = stiff_blocks.shape
    n, zn = lax.axis_size("sector"), lax.axis_size("row")
    sectors_all = sec * n
    slots = sec // 2
    table = coefficients(harmonic_table, sectors_all).reshape(n, slots, 2, sectors_all)
    table = table.transpose(1, 0, 2, 3).reshape(slots, 2 * n, sectors_all)
    table = jnp.pad(table, ((0, 0), (0, LANES - 2 * n), (0, LANES - sectors_all)))
    part = rows // n
    chunk = part // CHUNKS
    halo = (nband // 2) * blk
    total = 2 * modes
    own_rows = total // zn
    bf16, f32 = jnp.bfloat16, jnp.float32
    dma = pltpu.SemaphoreType.DMA
    vmem = pl.BlockSpec(memory_space=pltpu.VMEM)
    hbm = pl.BlockSpec(memory_space=pl.ANY)
    out = jax.ShapeDtypeStruct((slots, own_rows, total), f32)
    return pl.pallas_call(
        functools.partial(kernel, (n, zn, sec, rows, modes, nblk, nband, blk)),
        out_shape=(out, out),
        in_specs=[vmem, hbm, hbm, hbm],
        out_specs=(vmem, vmem),
        scratch_shapes=[
            pltpu.VMEM((CHUNKS, sectors_all, chunk, modes), bf16),
            pltpu.VMEM((CHUNKS, slots, 2 * n, chunk, modes), bf16),
            pltpu.VMEM((slots, 2, rows + 2 * halo, modes), bf16),
            pltpu.VMEM((total, rows), bf16),
            pltpu.VMEM((rows, 2 * total), bf16),
            pltpu.VMEM((2, nblk, nband, blk, blk), bf16),
            pltpu.VMEM((total, 2 * total), f32),
            pltpu.VMEM((slots, total, 2 * total), bf16),
            pltpu.VMEM((slots, zn - 1, own_rows, 2 * total), bf16),
            pltpu.VMEM((slots, 2, 2 * n * PACK, sectors_all * PACK), bf16),
            dma((CHUNKS, n)), dma((CHUNKS, n)), dma((CHUNKS,)),
            dma((CHUNKS, slots, n)), dma((CHUNKS, slots, n)), dma((CHUNKS, slots)),
            dma((slots, 2)), dma((slots, 2)),
            dma((slots, zn)), dma((slots, zn)),
            dma((2,)),
        ],
        compiler_params=pltpu.CompilerParams(
            collective_id=0, has_side_effects=True, vmem_limit_bytes=60 * 1024 * 1024),
    )(table, psi_sectors, stiff_blocks, mass_blocks)


def solution(mesh):
    placed = (P("sector", "row", None), P("row", None, None, None), P("row", None, None, None), P())
    return jax.shard_map(
        per_device,
        mesh=mesh,
        in_specs=placed,
        out_specs=(P("sector", "row", None), P("sector", "row", None)),
        check_vma=False,
    )
```

```python
import functools
import math

import jax
import jax.numpy as jnp
from jax import lax
from jax.experimental import pallas as pl
from jax.experimental.pallas import tpu as pltpu
from jax.sharding import PartitionSpec as P

MESH = pl.DeviceIdType.MESH
LANES = 128
PACK = 16
CHUNKS = 4


def flipped(index, step, count):
    total, bit = 0, 1
    while bit < count:
        total = total + bit * lax.rem(lax.div(index, bit) + (step // bit) % 2, 2)
        bit *= 2
    return total


def kernel(cfg, table_ref, psi_ref, stiff_ref, mass_ref, out_k, out_m,
           x_buf, h_buf, p_buf, pt_buf, y_buf, band, g_f32, g_send, g_recv, weights,
           s1, r1, l1, sp, rp, lp, s2, r2, l2, sh, rh, s3, r3, lb):
    n, zn, sec, rows, modes, nblk, nband, blk = cfg
    slots = sec // 2
    part = rows // n
    chunk = part // CHUNKS
    reach = nband // 2
    halo = reach * blk
    total = 2 * modes
    own_rows = total // zn
    halves = modes // LANES
    cols = total // LANES
    groups = slots * cols
    sectors_all = n * sec
    d = lax.axis_index("sector")
    z = lax.axis_index("row")
    order = [j for j in (2, 4, 6, 3, 5, 7) if j < n] + [1]
    order += [j for j in range(1, n) if j not in order]

    barrier = pltpu.get_barrier_semaphore()
    for j in order:
        pl.semaphore_signal(barrier, inc=1, device_id={"sector": flipped(d, j, n)}, device_id_type=MESH)
    for j in range(1, zn):
        pl.semaphore_signal(barrier, inc=1, device_id={"row": lax.rem(z + j, zn)}, device_id_type=MESH)
    pl.semaphore_wait(barrier, n - 1 + zn - 1)

    def first(q, j):
        target = flipped(d, j, n)
        return pltpu.make_async_remote_copy(
            src_ref=psi_ref.at[:, pl.ds(target * part + q * chunk, chunk), :],
            dst_ref=x_buf.at[q, pl.ds(d * sec, sec)],
            send_sem=s1.at[q, j], recv_sem=r1.at[q, j],
            device_id={"sector": target}, device_id_type=MESH)

    def first_own(q):
        return pltpu.make_async_copy(
            psi_ref.at[:, pl.ds(d * part + q * chunk, chunk), :],
            x_buf.at[q, pl.ds(d * sec, sec)], l1.at[q])

    def early(q, j):
        target = flipped(d, j, n)
        return pltpu.make_async_remote_copy(
            src_ref=h_buf.at[pl.ds(0, halves), target, pl.ds(q * chunk, chunk), :],
            dst_ref=p_buf.at[pl.ds(0, halves), pl.ds(halo + d * part + q * chunk, chunk), :],
            send_sem=sp.at[q, j], recv_sem=rp.at[q, j],
            device_id={"sector": target}, device_id_type=MESH)

    def early_own(q):
        return pltpu.make_async_copy(
            h_buf.at[pl.ds(0, halves), d, pl.ds(q * chunk, chunk), :],
            p_buf.at[pl.ds(0, halves), pl.ds(halo + d * part + q * chunk, chunk), :], lp.at[q])

    def second(g, j):
        target = flipped(d, j, n)
        return pltpu.make_async_remote_copy(
            src_ref=h_buf.at[g, target],
            dst_ref=p_buf.at[g, pl.ds(halo + d * part, part), :],
            send_sem=s2.at[g, j], recv_sem=r2.at[g, j],
            device_id={"sector": target}, device_id_type=MESH)

    def second_own(g):
        return pltpu.make_async_copy(
            h_buf.at[g, d], p_buf.at[g, pl.ds(halo + d * part, part), :], l2.at[g])

    def second_start(g):
        for j in order:
            second(g, j).start()
        second_own(g).start()

    def edge(g, up):
        source = rows if up else halo
        dest = 0 if up else halo + rows
        target = lax.rem(z + (1 if up else zn - 1), zn)
        return pltpu.make_async_remote_copy(
            src_ref=p_buf.at[g, pl.ds(source, halo), :],
            dst_ref=p_buf.at[g, pl.ds(dest, halo), :],
            send_sem=sh.at[g, int(up)], recv_sem=rh.at[g, int(up)],
            device_id={"row": target}, device_id_type=MESH)

    def row_group(device):
        return lax.div(device * own_rows, LANES)

    def third(h, j, c, whole):
        target = lax.rem(z + j, zn)
        start, width = (0, (c + 1) * 2 * LANES) if whole else (c * 2 * LANES, 2 * LANES)
        return pltpu.make_async_remote_copy(
            src_ref=g_send.at[h, pl.ds(target * own_rows, own_rows), pl.ds(start, width)],
            dst_ref=g_recv.at[h, j - 1, :, pl.ds(start, width)],
            send_sem=s3.at[h, j, c], recv_sem=r3.at[h, j, c],
            device_id={"row": target}, device_id_type=MESH)

    def third_do(h, c, what):
        for j in range(1, zn):
            held = row_group(z if what == "wait_recv" else lax.rem(z + j, zn))

            @pl.when(held == c)
            def _():
                getattr(third(h, j, c, True), what)()

            @pl.when(held < c)
            def _():
                getattr(third(h, j, c, False), what)()

    @pl.loop(0, CHUNKS)
    def _(q):
        for j in order:
            first(q, j).start()
        first_own(q).start()

    band_copies = [pltpu.make_async_copy(stiff_ref, band.at[0], lb.at[0]),
                   pltpu.make_async_copy(mass_ref, band.at[1], lb.at[1])]
    for copy in band_copies:
        copy.start()

    @pl.when(z == 0)
    def _():
        @pl.loop(0, groups)
        def _(g):
            p_buf[g, pl.ds(0, halo), :] = jnp.zeros((halo, LANES), p_buf.dtype)

    @pl.when(z == zn - 1)
    def _():
        @pl.loop(0, groups)
        def _(g):
            p_buf[g, pl.ds(halo + rows, halo), :] = jnp.zeros((halo, LANES), p_buf.dtype)

    wide_rows, wide_cols = 2 * n * PACK, sectors_all * PACK

    def spread(shape, long):
        return ((lax.broadcasted_iota(jnp.int32, shape, long) >> 4) == lax.broadcasted_iota(
            jnp.int32, shape, 1 - long)).astype(jnp.float32).astype(jnp.bfloat16)

    spread_rows = spread((wide_rows, LANES), 0)
    spread_cols = spread((LANES, wide_cols), 1)
    same = ((lax.broadcasted_iota(jnp.int32, (wide_rows, wide_cols), 0) & (PACK - 1))
            == (lax.broadcasted_iota(jnp.int32, (wide_rows, wide_cols), 1) & (PACK - 1)))
    line = lax.broadcasted_iota(jnp.int32, (LANES, LANES), 0)
    sector = lax.broadcasted_iota(jnp.int32, (LANES, LANES), 1)
    for h in range(slots):
        pair = jnp.zeros((LANES, LANES), jnp.int32)
        for e in range(n):
            pair = jnp.where((line == e) | (line == n + e), table_ref[e * slots + h], pair)
        lone = pair == 0
        upper = line >= n
        turns = jnp.where(lone & upper, sectors_all // 2, pair) * sector
        turns = turns + jnp.where(upper & jnp.logical_not(lone), sectors_all - sectors_all // 4, 0)
        turns = turns & (sectors_all - 1)
        scale = jnp.where(lone, math.sqrt(1.0 / sectors_all), math.sqrt(2.0 / sectors_all))
        value = scale * jnp.cos(turns.astype(jnp.float32) * (2.0 * math.pi / sectors_all))
        high = value.astype(jnp.bfloat16)
        low = (value - high.astype(jnp.float32)).astype(jnp.bfloat16)
        for index, piece in enumerate((high, low)):
            tall = jnp.dot(spread_rows, piece, preferred_element_type=jnp.float32).astype(jnp.bfloat16)
            full = jnp.dot(tall, spread_cols, preferred_element_type=jnp.float32)
            weights[h, index] = jnp.where(same, full, 0.0).astype(jnp.bfloat16)

    @pl.loop(0, CHUNKS)
    def _(q):
        for j in order:
            first(q, j).wait_recv()
        first_own(q).wait()

        @pl.loop(0, chunk // PACK)
        def _(t):
            x = x_buf[q, :, pl.ds(pl.multiple_of(t * PACK, PACK), PACK), :].reshape(wide_cols, modes)
            at = pl.ds(pl.multiple_of(q * chunk + t * PACK, PACK), PACK)
            for h in range(slots):
                value = (jnp.dot(weights[h, 0], x, preferred_element_type=jnp.float32)
                         + jnp.dot(weights[h, 1], x, preferred_element_type=jnp.float32)).astype(jnp.bfloat16)
                for c in range(cols):
                    k, half = c // halves, c % halves
                    h_buf[h * cols + c, :, at, :] = value[
                        k * n * PACK:(k + 1) * n * PACK, half * LANES:(half + 1) * LANES].reshape(n, PACK, LANES)

        for j in order:
            early(q, j).start()
        early_own(q).start()

    second_start(halves)

    for copy in band_copies:
        copy.wait()

    def block_row(g, c, i):
        at = pl.ds(pl.multiple_of(i * blk, blk), blk)
        blocks = jnp.concatenate(
            [jnp.concatenate([band[which, i, k] for k in range(nband)], axis=1) for which in range(2)], axis=0)
        window = p_buf[g, pl.ds(pl.multiple_of(i * blk, blk), nband * blk), :]
        image = jnp.dot(blocks, window, preferred_element_type=jnp.float32).astype(jnp.bfloat16)
        y_buf[at, c * 2 * LANES:c * 2 * LANES + LANES] = image[:blk]
        y_buf[at, c * 2 * LANES + LANES:(c + 1) * 2 * LANES] = image[blk:]
        pt_buf[c * LANES:(c + 1) * LANES, at] = window[halo:halo + blk].T

    def gram(h, first_row, row_count, c):
        span = slice(c * 2 * LANES, (c + 1) * 2 * LANES)
        value = jnp.dot(pt_buf[first_row:first_row + row_count, :], y_buf[:, span],
                        preferred_element_type=jnp.float32)
        g_f32[first_row:first_row + row_count, span] = value
        g_send[h, first_row:first_row + row_count, span] = value.astype(jnp.bfloat16)

    @pl.loop(0, slots)
    def _(h):
        for c in range(cols):
            g = h * cols + c

            def arrived():
                for j in order:
                    second(g, j).wait_recv()
                second_own(g).wait()

            if c == 0:
                @pl.when(h == 0)
                def _():
                    @pl.loop(0, CHUNKS)
                    def _(q):
                        for j in order:
                            early(q, j).wait_recv()
                        early_own(q).wait()

                    second_start(halves + 1)
            if c < halves:
                pl.when(h > 0)(arrived)
            else:
                arrived()

            @pl.when((g >= halves) & (g + 2 < groups))
            def _():
                second_start(g + 2)

            @pl.when(z < zn - 1)
            def _():
                edge(g, True).start()

            @pl.when(z > 0)
            def _():
                edge(g, False).start()

            @pl.loop(reach, nblk - reach)
            def _(i):
                block_row(g, c, i)

            @pl.when(z > 0)
            def _():
                edge(g, True).wait_recv()

            @pl.when(z < zn - 1)
            def _():
                edge(g, False).wait_recv()

            @pl.loop(0, 2 * reach)
            def _(i):
                block_row(g, c, lax.rem(i + nblk - reach, nblk))

            for b in range(c):
                gram(h, c * LANES, LANES, b)
            gram(h, 0, (c + 1) * LANES, c)
            third_do(h, c, "start")

        mine = pl.ds(pl.multiple_of(z * own_rows, own_rows), own_rows)
        for c in range(cols):
            out_k[h, :, c * LANES:(c + 1) * LANES] = g_f32[mine, c * 2 * LANES:c * 2 * LANES + LANES]
            out_m[h, :, c * LANES:(c + 1) * LANES] = g_f32[mine, c * 2 * LANES + LANES:(c + 1) * 2 * LANES]

    @pl.loop(0, slots)
    def _(h):
        for c in range(cols):
            third_do(h, c, "wait_recv")
        for c in range(cols):
            for which, out in enumerate((out_k, out_m)):
                start = (2 * c + which) * LANES
                value = out[h, :, c * LANES:(c + 1) * LANES]
                for j in range(1, zn):
                    value = value + g_recv[h, j - 1, :, start:start + LANES].astype(jnp.float32)
                out[h, :, c * LANES:(c + 1) * LANES] = value

    @pl.loop(0, CHUNKS)
    def _(q):
        for j in order:
            first(q, j).wait_send()
            early(q, j).wait_send()

    @pl.loop(halves, groups)
    def _(g):
        for j in order:
            second(g, j).wait_send()

    @pl.loop(0, groups)
    def _(g):
        @pl.when(z < zn - 1)
        def _():
            edge(g, True).wait_send()

        @pl.when(z > 0)
        def _():
            edge(g, False).wait_send()

    @pl.loop(0, slots)
    def _(h):
        for c in range(cols):
            third_do(h, c, "wait_send")


def per_device(psi_sectors, stiff_blocks, mass_blocks, harmonic_table):
    sec, rows, modes = psi_sectors.shape
    nblk, nband, blk, _ = stiff_blocks.shape
    n, zn = lax.axis_size("sector"), lax.axis_size("row")
    sectors_all = sec * n
    slots = sec // 2
    part = rows // n
    chunk = part // CHUNKS
    halo = (nband // 2) * blk
    total = 2 * modes
    cols = total // LANES
    own_rows = total // zn
    bf16, f32 = jnp.bfloat16, jnp.float32
    dma = pltpu.SemaphoreType.DMA
    vmem = pl.BlockSpec(memory_space=pltpu.VMEM)
    hbm = pl.BlockSpec(memory_space=pl.ANY)
    out = jax.ShapeDtypeStruct((slots, own_rows, total), f32)
    return pl.pallas_call(
        functools.partial(kernel, (n, zn, sec, rows, modes, nblk, nband, blk)),
        out_shape=(out, out),
        in_specs=[pl.BlockSpec(memory_space=pltpu.SMEM), hbm, hbm, hbm],
        out_specs=(vmem, vmem),
        scratch_shapes=[
            pltpu.VMEM((CHUNKS, sectors_all, chunk, modes), bf16),
            pltpu.VMEM((slots * cols, n, part, LANES), bf16),
            pltpu.VMEM((slots * cols, rows + 2 * halo, LANES), bf16),
            pltpu.VMEM((total, rows), bf16),
            pltpu.VMEM((rows, 2 * total), bf16),
            pltpu.VMEM((2, nblk, nband, blk, blk), bf16),
            pltpu.VMEM((total, 2 * total), f32),
            pltpu.VMEM((slots, total, 2 * total), bf16),
            pltpu.VMEM((slots, zn - 1, own_rows, 2 * total), bf16),
            pltpu.VMEM((slots, 2, 2 * n * PACK, sectors_all * PACK), bf16),
            dma((CHUNKS, n)), dma((CHUNKS, n)), dma((CHUNKS,)),
            dma((CHUNKS, n)), dma((CHUNKS, n)), dma((CHUNKS,)),
            dma((slots * cols, n)), dma((slots * cols, n)), dma((slots * cols,)),
            dma((slots * cols, 2)), dma((slots * cols, 2)),
            dma((slots, zn, cols)), dma((slots, zn, cols)),
            dma((2,)),
        ],
        compiler_params=pltpu.CompilerParams(
            collective_id=0, has_side_effects=True, vmem_limit_bytes=60 * 1024 * 1024),
    )(harmonic_table, psi_sectors, stiff_blocks, mass_blocks)


def solution(mesh):
    placed = (P("sector", "row", None), P("row", None, None, None), P("row", None, None, None), P())
    return jax.shard_map(
        per_device,
        mesh=mesh,
        in_specs=placed,
        out_specs=(P("sector", "row", None), P("sector", "row", None)),
        check_vma=False,
    )
```

```python
import functools
import math

import jax
import jax.numpy as jnp
from jax import lax
from jax.experimental import pallas as pl
from jax.experimental.pallas import tpu as pltpu
from jax.sharding import PartitionSpec as P

MESH = pl.DeviceIdType.MESH
LANES = 128
PACK = 16
CHUNKS = 4


def flipped(index, step, count):
    total, bit = 0, 1
    while bit < count:
        total = total + bit * lax.rem(lax.div(index, bit) + (step // bit) % 2, 2)
        bit *= 2
    return total


def kernel(cfg, table_ref, psi_ref, stiff_ref, mass_ref, out_k, out_m,
           x_buf, h_buf, p_buf, pt_buf, y_buf, band, g_f32, g_send, g_recv, weights,
           s1, r1, l1, sp, rp, lp, s2, r2, l2, sh, rh, s3, r3, lb):
    n, zn, sec, rows, modes, nblk, nband, blk = cfg
    slots = sec // 2
    part = rows // n
    chunk = part // CHUNKS
    reach = nband // 2
    halo = reach * blk
    total = 2 * modes
    own_rows = total // zn
    halves = modes // LANES
    cols = total // LANES
    groups = slots * cols
    place = [(c % 2) * (cols // 2) + c // 2 for c in range(cols)]
    turn = [place.index(p) for p in range(cols)]
    sectors_all = n * sec
    d = lax.axis_index("sector")
    z = lax.axis_index("row")
    order = [j for j in (2, 4, 6, 3, 5, 7) if j < n] + [1]
    order += [j for j in range(1, n) if j not in order]

    barrier = pltpu.get_barrier_semaphore()
    for j in order:
        pl.semaphore_signal(barrier, inc=1, device_id={"sector": flipped(d, j, n)}, device_id_type=MESH)
    for j in range(1, zn):
        pl.semaphore_signal(barrier, inc=1, device_id={"row": lax.rem(z + j, zn)}, device_id_type=MESH)
    pl.semaphore_wait(barrier, n - 1 + zn - 1)

    def first(q, j):
        target = flipped(d, j, n)
        return pltpu.make_async_remote_copy(
            src_ref=psi_ref.at[:, pl.ds(target * part + q * chunk, chunk), :],
            dst_ref=x_buf.at[q, pl.ds(d * sec, sec)],
            send_sem=s1.at[q, j], recv_sem=r1.at[q, j],
            device_id={"sector": target}, device_id_type=MESH)

    def first_own(q):
        return pltpu.make_async_copy(
            psi_ref.at[:, pl.ds(d * part + q * chunk, chunk), :],
            x_buf.at[q, pl.ds(d * sec, sec)], l1.at[q])

    def early(q, j):
        target = flipped(d, j, n)
        return pltpu.make_async_remote_copy(
            src_ref=h_buf.at[pl.ds(0, halves), target, pl.ds(q * chunk, chunk), :],
            dst_ref=p_buf.at[pl.ds(0, halves), pl.ds(halo + d * part + q * chunk, chunk), :],
            send_sem=sp.at[q, j], recv_sem=rp.at[q, j],
            device_id={"sector": target}, device_id_type=MESH)

    def early_own(q):
        return pltpu.make_async_copy(
            h_buf.at[pl.ds(0, halves), d, pl.ds(q * chunk, chunk), :],
            p_buf.at[pl.ds(0, halves), pl.ds(halo + d * part + q * chunk, chunk), :], lp.at[q])

    def second(g, j):
        target = flipped(d, j, n)
        return pltpu.make_async_remote_copy(
            src_ref=h_buf.at[g, target],
            dst_ref=p_buf.at[g, pl.ds(halo + d * part, part), :],
            send_sem=s2.at[g, j], recv_sem=r2.at[g, j],
            device_id={"sector": target}, device_id_type=MESH)

    def second_own(g):
        return pltpu.make_async_copy(
            h_buf.at[g, d], p_buf.at[g, pl.ds(halo + d * part, part), :], l2.at[g])

    def second_start(g):
        for j in order:
            second(g, j).start()
        second_own(g).start()

    def edge(g, up):
        source = rows if up else halo
        dest = 0 if up else halo + rows
        target = lax.rem(z + (1 if up else zn - 1), zn)
        return pltpu.make_async_remote_copy(
            src_ref=p_buf.at[g, pl.ds(source, halo), :],
            dst_ref=p_buf.at[g, pl.ds(dest, halo), :],
            send_sem=sh.at[g, int(up)], recv_sem=rh.at[g, int(up)],
            device_id={"row": target}, device_id_type=MESH)

    def row_group(device):
        group = lax.div(device * own_rows, LANES)
        return lax.rem(group, 2) * (cols // 2) + lax.div(group, 2)

    def row_start(device):
        return row_group(device) * LANES + lax.rem(device * own_rows, LANES)

    def third(h, j, c, whole):
        target = lax.rem(z + j, zn)
        start, width = (0, (c + 1) * 2 * LANES) if whole else (c * 2 * LANES, 2 * LANES)
        return pltpu.make_async_remote_copy(
            src_ref=g_send.at[h, pl.ds(row_start(target), own_rows), pl.ds(start, width)],
            dst_ref=g_recv.at[h, j - 1, :, pl.ds(start, width)],
            send_sem=s3.at[h, j, c], recv_sem=r3.at[h, j, c],
            device_id={"row": target}, device_id_type=MESH)

    def third_do(h, c, what):
        for j in range(1, zn):
            held = row_group(z if what == "wait_recv" else lax.rem(z + j, zn))

            @pl.when(held == c)
            def _():
                getattr(third(h, j, c, True), what)()

            @pl.when(held < c)
            def _():
                getattr(third(h, j, c, False), what)()

    @pl.loop(0, CHUNKS)
    def _(q):
        for j in order:
            first(q, j).start()
        first_own(q).start()

    band_copies = [pltpu.make_async_copy(stiff_ref, band.at[0], lb.at[0]),
                   pltpu.make_async_copy(mass_ref, band.at[1], lb.at[1])]
    for copy in band_copies:
        copy.start()

    @pl.when(z == 0)
    def _():
        @pl.loop(0, groups)
        def _(g):
            p_buf[g, pl.ds(0, halo), :] = jnp.zeros((halo, LANES), p_buf.dtype)

    @pl.when(z == zn - 1)
    def _():
        @pl.loop(0, groups)
        def _(g):
            p_buf[g, pl.ds(halo + rows, halo), :] = jnp.zeros((halo, LANES), p_buf.dtype)

    wide_rows, wide_cols = 2 * n * PACK, sectors_all * PACK

    def spread(shape, long):
        return ((lax.broadcasted_iota(jnp.int32, shape, long) >> 4) == lax.broadcasted_iota(
            jnp.int32, shape, 1 - long)).astype(jnp.float32).astype(jnp.bfloat16)

    spread_rows = spread((wide_rows, LANES), 0)
    spread_cols = spread((LANES, wide_cols), 1)
    same = ((lax.broadcasted_iota(jnp.int32, (wide_rows, wide_cols), 0) & (PACK - 1))
            == (lax.broadcasted_iota(jnp.int32, (wide_rows, wide_cols), 1) & (PACK - 1)))
    line = lax.broadcasted_iota(jnp.int32, (LANES, LANES), 0)
    sector = lax.broadcasted_iota(jnp.int32, (LANES, LANES), 1)
    for h in range(slots):
        pair = jnp.zeros((LANES, LANES), jnp.int32)
        for e in range(n):
            pair = jnp.where((line == e) | (line == n + e), table_ref[e * slots + h], pair)
        lone = pair == 0
        upper = line >= n
        turns = jnp.where(lone & upper, sectors_all // 2, pair) * sector
        turns = turns + jnp.where(upper & jnp.logical_not(lone), sectors_all - sectors_all // 4, 0)
        turns = turns & (sectors_all - 1)
        scale = jnp.where(lone, math.sqrt(1.0 / sectors_all), math.sqrt(2.0 / sectors_all))
        value = scale * jnp.cos(turns.astype(jnp.float32) * (2.0 * math.pi / sectors_all))
        high = value.astype(jnp.bfloat16)
        low = (value - high.astype(jnp.float32)).astype(jnp.bfloat16)
        for index, piece in enumerate((high, low)):
            tall = jnp.dot(spread_rows, piece, preferred_element_type=jnp.float32).astype(jnp.bfloat16)
            full = jnp.dot(tall, spread_cols, preferred_element_type=jnp.float32)
            weights[h, index] = jnp.where(same, full, 0.0).astype(jnp.bfloat16)

    @pl.loop(0, CHUNKS)
    def _(q):
        for j in order:
            first(q, j).wait_recv()
        first_own(q).wait()

        @pl.loop(0, chunk // PACK)
        def _(t):
            x = x_buf[q, :, pl.ds(pl.multiple_of(t * PACK, PACK), PACK), :].reshape(wide_cols, modes)
            at = pl.ds(pl.multiple_of(q * chunk + t * PACK, PACK), PACK)
            for h in range(slots):
                value = (jnp.dot(weights[h, 0], x, preferred_element_type=jnp.float32)
                         + jnp.dot(weights[h, 1], x, preferred_element_type=jnp.float32)).astype(jnp.bfloat16)
                for c in range(cols):
                    k, half = turn[c] // halves, turn[c] % halves
                    h_buf[h * cols + c, :, at, :] = value[
                        k * n * PACK:(k + 1) * n * PACK, half * LANES:(half + 1) * LANES].reshape(n, PACK, LANES)

        for j in order:
            early(q, j).start()
        early_own(q).start()

    second_start(halves)

    for copy in band_copies:
        copy.wait()

    def block_row(g, c, i):
        at = pl.ds(pl.multiple_of(i * blk, blk), blk)
        blocks = jnp.concatenate(
            [jnp.concatenate([band[which, i, k] for k in range(nband)], axis=1) for which in range(2)], axis=0)
        window = p_buf[g, pl.ds(pl.multiple_of(i * blk, blk), nband * blk), :]
        image = jnp.dot(blocks, window, preferred_element_type=jnp.float32).astype(jnp.bfloat16)
        y_buf[at, c * 2 * LANES:c * 2 * LANES + LANES] = image[:blk]
        y_buf[at, c * 2 * LANES + LANES:(c + 1) * 2 * LANES] = image[blk:]
        pt_buf[c * LANES:(c + 1) * LANES, at] = window[halo:halo + blk].T

    def gram(h, first_row, row_count, c):
        span = slice(c * 2 * LANES, (c + 1) * 2 * LANES)
        value = jnp.dot(pt_buf[first_row:first_row + row_count, :], y_buf[:, span],
                        preferred_element_type=jnp.float32)
        g_f32[first_row:first_row + row_count, span] = value
        g_send[h, first_row:first_row + row_count, span] = value.astype(jnp.bfloat16)

    def take(g, c, begin):
        def arrived():
            for j in order:
                second(g, j).wait_recv()
            second_own(g).wait()

        if begin and c == 0:
            @pl.loop(0, CHUNKS)
            def _(q):
                for j in order:
                    early(q, j).wait_recv()
                early_own(q).wait()

            second_start(halves + 1)
        elif c >= halves:
            arrived()
        else:
            pl.when(g >= halves)(arrived)

        @pl.when((g >= halves) & (g + 2 < groups))
        def _():
            second_start(g + 2)

        @pl.when(z < zn - 1)
        def _():
            edge(g, True).start()

        @pl.when(z > 0)
        def _():
            edge(g, False).start()

    take(0, 0, True)

    @pl.loop(0, slots)
    def _(h):
        for c in range(cols):
            g = h * cols + c

            @pl.loop(reach, nblk - reach)
            def _(i):
                block_row(g, c, i)

            @pl.when(z > 0)
            def _():
                edge(g, True).wait_recv()

            @pl.when(z < zn - 1)
            def _():
                edge(g, False).wait_recv()

            @pl.loop(0, 2 * reach)
            def _(i):
                block_row(g, c, lax.rem(i + nblk - reach, nblk))

            for b in range(c):
                gram(h, c * LANES, LANES, b)
            gram(h, 0, (c + 1) * LANES, c)
            if c + 1 < cols:
                take(g + 1, c + 1, False)
            else:
                @pl.when(h + 1 < slots)
                def _():
                    take(g + 1, 0, False)
            third_do(h, c, "start")

        mine = pl.ds(pl.multiple_of(row_start(z), own_rows), own_rows)
        for c in range(cols):
            out_k[h, :, turn[c] * LANES:(turn[c] + 1) * LANES] = g_f32[mine, c * 2 * LANES:c * 2 * LANES + LANES]
            out_m[h, :, turn[c] * LANES:(turn[c] + 1) * LANES] = g_f32[mine, c * 2 * LANES + LANES:(c + 1) * 2 * LANES]

    @pl.loop(0, slots)
    def _(h):
        for c in range(cols):
            third_do(h, c, "wait_recv")
        for c in range(cols):
            for which, out in enumerate((out_k, out_m)):
                start = (2 * c + which) * LANES
                place_out = slice(turn[c] * LANES, (turn[c] + 1) * LANES)
                value = out[h, :, place_out]
                for j in range(1, zn):
                    value = value + g_recv[h, j - 1, :, start:start + LANES].astype(jnp.float32)
                out[h, :, place_out] = value

    @pl.loop(0, CHUNKS)
    def _(q):
        for j in order:
            first(q, j).wait_send()
            early(q, j).wait_send()

    @pl.loop(halves, groups)
    def _(g):
        for j in order:
            second(g, j).wait_send()

    @pl.loop(0, groups)
    def _(g):
        @pl.when(z < zn - 1)
        def _():
            edge(g, True).wait_send()

        @pl.when(z > 0)
        def _():
            edge(g, False).wait_send()

    @pl.loop(0, slots)
    def _(h):
        for c in range(cols):
            third_do(h, c, "wait_send")


def per_device(psi_sectors, stiff_blocks, mass_blocks, harmonic_table):
    sec, rows, modes = psi_sectors.shape
    nblk, nband, blk, _ = stiff_blocks.shape
    n, zn = lax.axis_size("sector"), lax.axis_size("row")
    sectors_all = sec * n
    slots = sec // 2
    part = rows // n
    chunk = part // CHUNKS
    halo = (nband // 2) * blk
    total = 2 * modes
    cols = total // LANES
    own_rows = total // zn
    bf16, f32 = jnp.bfloat16, jnp.float32
    dma = pltpu.SemaphoreType.DMA
    vmem = pl.BlockSpec(memory_space=pltpu.VMEM)
    hbm = pl.BlockSpec(memory_space=pl.ANY)
    out = jax.ShapeDtypeStruct((slots, own_rows, total), f32)
    return pl.pallas_call(
        functools.partial(kernel, (n, zn, sec, rows, modes, nblk, nband, blk)),
        out_shape=(out, out),
        in_specs=[pl.BlockSpec(memory_space=pltpu.SMEM), hbm, hbm, hbm],
        out_specs=(vmem, vmem),
        scratch_shapes=[
            pltpu.VMEM((CHUNKS, sectors_all, chunk, modes), bf16),
            pltpu.VMEM((slots * cols, n, part, LANES), bf16),
            pltpu.VMEM((slots * cols, rows + 2 * halo, LANES), bf16),
            pltpu.VMEM((total, rows), bf16),
            pltpu.VMEM((rows, 2 * total), bf16),
            pltpu.VMEM((2, nblk, nband, blk, blk), bf16),
            pltpu.VMEM((total, 2 * total), f32),
            pltpu.VMEM((slots, total, 2 * total), bf16),
            pltpu.VMEM((slots, zn - 1, own_rows, 2 * total), bf16),
            pltpu.VMEM((slots, 2, 2 * n * PACK, sectors_all * PACK), bf16),
            dma((CHUNKS, n)), dma((CHUNKS, n)), dma((CHUNKS,)),
            dma((CHUNKS, n)), dma((CHUNKS, n)), dma((CHUNKS,)),
            dma((slots * cols, n)), dma((slots * cols, n)), dma((slots * cols,)),
            dma((slots * cols, 2)), dma((slots * cols, 2)),
            dma((slots, zn, cols)), dma((slots, zn, cols)),
            dma((2,)),
        ],
        compiler_params=pltpu.CompilerParams(
            collective_id=0, has_side_effects=True, vmem_limit_bytes=60 * 1024 * 1024),
    )(harmonic_table, psi_sectors, stiff_blocks, mass_blocks)


def solution(mesh):
    placed = (P("sector", "row", None), P("row", None, None, None), P("row", None, None, None), P())
    return jax.shard_map(
        per_device,
        mesh=mesh,
        in_specs=placed,
        out_specs=(P("sector", "row", None), P("sector", "row", None)),
        check_vma=False,
    )
```
